1024 devices in a mesh: dp: 16 (over x_hi, y), mp: 64 (over x_lo, z, core).
Axes of the slice: x: 8 (x_hi: 2, x_lo: 4; x = x_hi * 4 + x_lo), y: 8, z: 8, core: 2. Of those that a mesh axis runs over, the one named last changes fastest.
Arguments:
- inputs: bfloat16 [2048, 6144], P('dp'), may hold values from -6 to 6
- pre_act: bfloat16 [2048, 12288], P('dp', 'mp'), may hold values from -6 to 6
- out_grad: bfloat16 [2048, 6144], P('dp'), may hold values from -6 to 6
- w_in: bfloat16 [6144, 12288], P(None, 'mp'), may hold values from -0.21875 to 0.21875
- w_out: bfloat16 [12288, 6144], P('mp'), may hold values from -0.0546875 to 0.0546875
- master_in: float32 [6144, 12288], P('dp', 'mp'), may hold values from -0.3 to 0.3
- master_out: float32 [12288, 6144], P('mp', 'dp'), may hold values from -0.3 to 0.3
- row_in: float32 [6144], P('dp'), may hold values from 25.6 to 1372.16
- col_in: float32 [12288], P('mp'), may hold values from 51 to 256
- row_out: float32 [12288], P('mp'), may hold values from 51.2 to 2744.32
- col_out: float32 [6144], P('dp'), may hold values from 102 to 512
Outputs:
- input_grad: bfloat16 [2048, 6144], P('dp', 'mp')
- new_master_in: float32 [6144, 12288], P('dp', 'mp')
- new_master_out: float32 [12288, 6144], P('mp', 'dp')
The draws below stay inside these ranges and needn't reach their ends.
All inputs are finite; a program needn't handle non-finite values.
Results may differ from the reference program's by a relative error of at most 0.012.
Values may be sent and summed in bfloat16 or wider, within the bound.
A program may use at most 64 MiB of HBM per device.

```python
import math
import jax
import jax.numpy as jnp
from jax import lax

D = 6144
FF = 12288
TOK_DEV = 128
TOKENS = 2048
N_DP = 16


def falling_factor(key, count, high, ratio):
    place = jnp.arange(count, dtype=jnp.float32) / float(count)
    noise = jax.random.uniform(key, (count,), jnp.float32, -0.28, 0.28)
    return high * jnp.exp(-jnp.log(ratio) * place + noise)


def draw_row_in(key, part):
    return falling_factor(jax.random.fold_in(key, 11), D, TOKENS * 0.5, 10.0)


def draw_row_out(key, part):
    return falling_factor(jax.random.fold_in(key, 23), FF, TOKENS * 1.0, 10.0)


def spiked(entries, key, source, target, blocks, factor):
    owner, partner = [(jnp.arange(entries.shape[position]) // (entries.shape[position] // blocks)).reshape([-1 if axis == position else 1 for axis in range(entries.ndim)]) for position in (source, target)]
    chosen = jax.random.permutation(key, blocks)[partner]
    strong = (owner == chosen) | (owner == (partner + blocks // 2) % blocks)
    return jnp.where(strong, factor * entries, entries)


def levels(rng, extent, cuts, least, high):
    loudness, own = 1.0, jax.random.fold_in(rng, 6)
    for position, blocks in cuts:
        heights = jnp.exp(jax.random.uniform(jax.random.fold_in(own, position), (blocks,), jnp.float32, least / len(cuts), high / len(cuts)))
        loudness = loudness * jnp.repeat(heights, extent[position] // blocks).reshape([-1 if axis == position else 1 for axis in range(len(extent))])
    return loudness


def scatter_about(stream_key, extent, width, most, shards=(), held_as=jnp.bfloat16):
    entries = width * jax.random.normal(stream_key, extent, jnp.float32)
    if shards:
        entries = entries * levels(stream_key, extent, shards, -0.22, 0.18)
    return jnp.clip(entries, -most, most).astype(held_as)


def noise_with(rng, dims, deviation, reach, cuts, heavy, held_as=jnp.bfloat16):
    drawn = deviation * jax.random.normal(rng, dims, jnp.float32)
    if cuts:
        drawn = drawn * levels(rng, dims, cuts, -0.22, 0.18)
    return jnp.clip(spiked(drawn, jax.random.fold_in(rng, 3), *heavy), -reach, reach).astype(held_as)


def setup_inputs(seed: int = 0) -> dict:
    keys = jax.random.split(jax.random.key(seed), 12)
    inputs = noise_with(keys[0], (TOKENS, D), 1.0, 6.0, ((0, 16),), (0, 1, 16, 2.0))
    pre_act = scatter_about(keys[1], (TOKENS, FF), 1.0, 6.0, ((0, 16), (1, 64)))
    out_grad = noise_with(keys[2], (TOKENS, D), 1.0, 6.0, ((0, 16),), (0, 1, 16, 2.0))
    w_in = noise_with(keys[3], (D, FF), D ** -0.5, 0.21875, ((1, 64),), (1, 0, 64, 4.0))
    w_out = scatter_about(keys[4], (FF, D), FF ** -0.5, 0.0546875, ((0, 64),))
    master_in = scatter_about(keys[5], (D, FF), 0.05, 0.3, ((0, 16), (1, 64)), jnp.float32)
    master_out = scatter_about(keys[6], (FF, D), 0.05, 0.3, ((0, 64), (1, 16)), jnp.float32)
    row_in = draw_row_in(jax.random.fold_in(keys[11], 71), 0)
    col_in = jnp.clip(jnp.exp(math.log(256.0) - 1.6133518 * jax.random.uniform(keys[8], (FF,), jnp.float32) ** levels(keys[8], (FF,), ((0, 64),), -0.2, 0.2)), 51.0, 256.0)
    row_out = draw_row_out(jax.random.fold_in(keys[11], 71), 0)
    col_out = jnp.clip(jnp.exp(math.log(512.0) - 1.6133518 * jax.random.uniform(keys[10], (D,), jnp.float32) ** levels(keys[10], (D,), ((0, 16),), -0.2, 0.2)), 102.0, 512.0)
    return dict(inputs=inputs, pre_act=pre_act, out_grad=out_grad, w_in=w_in, w_out=w_out, master_in=master_in, master_out=master_out, row_in=row_in, col_in=col_in, row_out=row_out, col_out=col_out)


decay_rate = 0.8
step_size = 0.05
tiny_square = 1e-30

def gelu_parts(pre):
    cumulative = 0.5 * (1.0 + jax.scipy.special.erf(pre * (1.0 / math.sqrt(2.0))))
    density = jnp.exp(-0.5 * pre * pre) * (1.0 / math.sqrt(2.0 * math.pi))
    return (pre * cumulative, cumulative + pre * density)

def adafactor(grad, master, row_state, col_state):
    square = grad * grad + tiny_square
    row_new = decay_rate * row_state + (1.0 - decay_rate) * lax.optimization_barrier(jnp.mean(square, axis=1))
    col_new = decay_rate * col_state + (1.0 - decay_rate) * lax.optimization_barrier(jnp.mean(square, axis=0))
    second = row_new[:, None] * col_new[None, :] / jnp.mean(row_new)
    update = grad / jnp.sqrt(second)
    return master - step_size * update

def reference(inputs, pre_act, out_grad, w_in, w_out, master_in, master_out, row_in, col_in, row_out, col_out):
    active, slope = gelu_parts(pre_act.astype(jnp.float32))
    hidden = active.astype(jnp.bfloat16)
    hid_grad = jnp.dot(out_grad, w_out.T, preferred_element_type=jnp.float32)
    pre_grad = (hid_grad * slope).astype(jnp.bfloat16)
    input_grad = jnp.dot(pre_grad, w_in.T, preferred_element_type=jnp.float32).astype(jnp.bfloat16)

    def group(totals, index):
        begin = (index * TOK_DEV).astype(jnp.int32)
        rows_x = lax.dynamic_slice_in_dim(inputs, begin, TOK_DEV, 0)
        rows_g = lax.dynamic_slice_in_dim(pre_grad, begin, TOK_DEV, 0)
        rows_h = lax.dynamic_slice_in_dim(hidden, begin, TOK_DEV, 0)
        rows_y = lax.dynamic_slice_in_dim(out_grad, begin, TOK_DEV, 0)
        part_in = jnp.dot(rows_x.T, rows_g, preferred_element_type=jnp.float32).astype(jnp.bfloat16)
        part_out = jnp.dot(rows_h.T, rows_y, preferred_element_type=jnp.float32).astype(jnp.bfloat16)
        part_in, part_out = lax.optimization_barrier((part_in, part_out))
        return ((totals[0] + part_in.astype(jnp.float32), totals[1] + part_out.astype(jnp.float32)), None)
    start_sums = (jnp.zeros((D, FF), jnp.float32), jnp.zeros((FF, D), jnp.float32))
    (grad_in, grad_out), _ = lax.scan(group, start_sums, jnp.arange(N_DP, dtype=jnp.int32))
    new_master_in = adafactor(grad_in, master_in, row_in, col_in)
    new_master_out = adafactor(grad_out, master_out, row_out, col_out)
    return (input_grad, new_master_in, new_master_out)
```

```python
import math

import jax
import jax.numpy as jnp
from jax import lax
from jax.experimental import pallas as pl
from jax.experimental.pallas import tpu as pltpu
from jax.sharding import PartitionSpec as P

MESH = pl.DeviceIdType.MESH
BF = jnp.bfloat16
F32 = jnp.float32
D = 6144
FF = 12288
TOK = 128
COLS = 384
HID = 192
OUTC = 96
RT = 16
DECAY = 0.8
STEP = 0.05
TINY = 1e-30


def xor2(a, k):
    return ((a // 2 + k // 2) % 2) * 2 + (a % 2 + k % 2) % 2


def slot(other, dy):
    dy = dy % 8
    chunk = (3 if dy % 2 else 0) if other else (2 if dy % 2 else 1)
    return (chunk * 4 + dy // 2) * TOK


def schedule(direction):
    last = (0, 1) if direction == 0 else (2, 3)
    return [(hop, k) for hop in (1, 2, 3) for k in range(4)] + [(4, k) for k in last]


def following(direction, n):
    if n < 8:
        return n + 4
    if n < 12:
        k = n - 8
        if direction == 0 and k < 2:
            return 12 + k
        if direction == 1 and k >= 2:
            return 12 + k - 2
    return None


KINDS = ((1, 0), (0, 0), (1, 1), (0, 1))


def kernel(
    x_hbm, pre_hbm, g_hbm, win_hbm, wout_hbm, min_hbm, mout_hbm, rin_hbm, cin_hbm, rout_hbm, cout_hbm,
    ig_out, nmi_out, nmo_out,
    pre_v, g_v, win_v, wout_v, min_v, mout_v, rin_v, cin_v, rout_v, cout_v,
    xg, hp, p_v, qown, a0s, a0r, a1s, a1r, a2s, a2r, fold, stw, sth, wr0, wr1, hr1, wr2, hr2, tr3,
    lsem, s1s, s1r, s2s, s2r, zs, zr, ys, yr, cs, cr, xs, xr,
    a0ss, a0rs, a1ss, a1rs, a2ss, a2rs, t0s, t0r, t1s, t1r, u1s, u1r, t2s, t2r, u2s, u2r, t3s, t3r,
):
    dp = lax.axis_index("dp")
    mp = lax.axis_index("mp")
    h, y = dp // 8, dp % 8
    a, z, c = mp // 16, (mp // 2) % 8, mp % 2
    x = h * 4 + a

    def at(xx, yy, zz, cc):
        xx, yy, zz = xx % 8, yy % 8, zz % 8
        return ((xx // 4) * 8 + yy, (xx % 4) * 16 + zz * 2 + cc)

    def remote(src, dst, ss, rs, dev):
        return pltpu.make_async_remote_copy(
            src_ref=src, dst_ref=dst, send_sem=ss, recv_sem=rs, device_id=dev, device_id_type=MESH
        )

    partner = at(x, y, z, 1 - c)
    loads = [
        pltpu.make_async_copy(s, d, lsem.at[i])
        for i, (s, d) in enumerate(
            (
                (pre_hbm, pre_v), (g_hbm, g_v), (wout_hbm, wout_v), (win_hbm, win_v), (min_hbm, min_v),
                (mout_hbm, mout_v), (rin_hbm, rin_v), (cin_hbm, cin_v), (rout_hbm, rout_v), (cout_hbm, cout_v),
            )
        )
    ]
    for cp in loads:
        cp.start()

    a_far = 3 - a
    x_far = (1 - h) * 4 + a_far
    greet = [at(x + k, y, z, c) for k in range(1, 8)]
    greet += [at(x, y + k, z, c) for k in range(1, 8)]
    greet += [at(x, y, z + k, c) for k in range(1, 8)]
    greet += [at(x, y, z + k, 1 - c) for k in range(8)]
    greet += [at(x_far, y + k, z, c) for k in range(1, 8)]
    barrier = pltpu.get_barrier_semaphore()
    for dev in greet:
        pl.semaphore_signal(barrier, inc=1, device_id=dev, device_id_type=MESH)

    loads[0].wait()
    pre = pre_v[...].astype(F32)
    cumulative = 0.5 * (1.0 + lax.erf(pre * (1.0 / math.sqrt(2.0))))
    density = jnp.exp(-0.5 * pre * pre) * (1.0 / math.sqrt(2.0 * math.pi))
    own = slot(0, 0)
    hp[1, :, own : own + TOK] = (pre * cumulative).astype(BF)
    slope = cumulative + pre * density

    pl.semaphore_wait(barrier, len(greet))

    near = (a + 1) // 2 % 2 == 1
    q_to = jnp.where(near, a, a_far)
    x_to = jnp.where(near, x, x_far)
    odd = q_to // 2

    def s1_copy(src, idx):
        y_to = (y - (2 * idx + odd)) % 8
        j = (x_to // 4) * 8 + y_to
        piece = src.at[pl.ds(pl.multiple_of(RT * z, RT), RT), pl.ds(pl.multiple_of(COLS * j, COLS), COLS)]
        return piece, xg.at[c, q_to, idx, z], at(x_to, y_to, z, c)

    def s1_start(src):
        for idx in range(4):
            piece, there, dev = s1_copy(src, idx)

            def far_copy():
                remote(piece, there, s1s.at[idx], s1r.at[idx], dev).start()

            if idx == 0:

                @pl.when(a == 1)
                def _():
                    pltpu.make_async_copy(piece, there, s1r.at[idx]).start()

                pl.when(a != 1)(far_copy)
            else:
                far_copy()

    @pl.when(c == 0)
    def _():
        s1_start(x_hbm)

    @pl.when(c == 1)
    def _():
        s1_start(g_hbm)

    def y_msg(d, n):
        hop, kind = schedule(d)[n]
        of, other = KINDS[kind]
        sgn = 1 if d == 0 else -1
        b, e = slot(other, -sgn * (hop - 1)), slot(other, -sgn * hop)
        return remote(
            hp.at[of, :, b : b + TOK], hp.at[of, :, e : e + TOK], ys.at[d, n], yr.at[d, n], at(x, y + sgn, z, c)
        )

    def cross(of):
        b, e = slot(0, 0), slot(1, 0)
        return remote(hp.at[of, :, b : b + TOK], hp.at[of, :, e : e + TOK], xs.at[of], xr.at[of], at(x + 4, y, z, c))

    cross(1).start()
    for d in (0, 1):
        y_msg(d, 0).start()

    loads[1].wait()
    loads[2].wait()
    hid_grad = lax.dot_general(wout_v[...], g_v[...], (((1,), (1,)), ((), ())), preferred_element_type=F32)
    pre_grad = hid_grad * slope
    hp[0, :, own : own + TOK] = pre_grad.astype(BF)
    p_v[...] = jnp.transpose(pre_grad).astype(BF)
    cross(0).start()
    for d in (0, 1):
        y_msg(d, 1).start()

    def piece_of(k, zo):
        return xg.at[c, xor2(a, k), :, zo % 8]

    def z_msg(d, n):
        hop, k = schedule(d)[n]
        sgn = 1 if d == 0 else -1
        ref = piece_of(k, z - sgn * (hop - 1))
        return remote(ref, ref, zs.at[d, n], zr.at[d, n], at(x, y, z + sgn, c))

    def share(k, rel):
        ref = piece_of(k, z + rel)
        return remote(ref, ref, cs.at[k, rel % 8], cr.at[k, rel % 8], partner)

    for idx in range(4):
        pltpu.make_async_copy(xg.at[c, a, idx, z], xg.at[c, a, idx, z], s1r.at[idx]).wait()

    def s2_msg(k):
        ref = piece_of(0, z)
        return remote(ref, ref, s2s.at[k - 1], s2r.at[k - 1], at(h * 4 + xor2(a, k), y, z, c))

    for k in (1, 2, 3):
        s2_msg(k).start()
    for k in range(4):
        if k:
            s2_msg(k).wait_recv()
        for d in (0, 1):
            z_msg(d, k).start()
        share(k, 0).start()

    cross(1).wait_recv()
    for d in (0, 1):
        y_msg(d, 2).start()

    loads[3].wait()

    def product(k, half):
        at_col = pl.multiple_of(1536 * xor2(a, k) + 768 * half, 128)
        return jnp.dot(p_v[...], win_v[:, pl.ds(at_col, 768)], preferred_element_type=F32)

    def a0_msg(k):
        return remote(a0s.at[k], a0r.at[k], a0ss.at[k], a0rs.at[k], partner)

    for k in (1, 2, 3, 0):
        a0s[k] = product(k, 1 - c).astype(BF)
        a0_msg(k).start()

    cross(0).wait_recv()
    for d in (0, 1):
        y_msg(d, 3).start()

    def tick(n):
        for d in (0, 1):
            hop, k = schedule(d)[n]
            sgn = 1 if d == 0 else -1
            after = following(d, n)
            z_msg(d, n).wait_recv()
            if after is not None:
                z_msg(d, after).start()
            share(k, -sgn * hop).start()
        for d in (0, 1):
            after = following(d, n)
            y_msg(d, n).wait_recv()
            if after is not None:
                y_msg(d, after).start()

    def a1_msg(k):
        return remote(
            a1s.at[k - 1], a1r.at[k - 1], a1ss.at[k - 1], a1rs.at[k - 1], at(h * 4 + xor2(a, k), y, z, c)
        )

    tick(0)
    for k in (1, 2, 3, 0):
        mine = product(k, c)
        a0_msg(k).wait_recv()
        mine = mine + a0r[k].astype(F32)
        if k:
            a1s[k - 1] = mine.astype(BF)
            a1_msg(k).start()
        else:
            qown[...] = mine
        tick({1: 1, 2: 2, 3: 3, 0: 4}[k])
    for n in range(5, 14):
        tick(n)
    for k in range(4):
        for rel in range(8):
            share(k, rel).wait_recv()

    def gradient(of):
        total = jnp.zeros((HID, COLS), F32)
        for q in range(4):
            total += jnp.dot(
                hp[of, :, 512 * q : 512 * (q + 1)], xg[of, q].reshape(512, COLS), preferred_element_type=F32
            )
        return total

    grad_in = gradient(0)
    grad_out = gradient(1)

    def thirds(v):
        return v[:, :128], v[:, 128:256], v[:, 256:]

    for cp in loads[4:]:
        cp.wait()
    fold[...] = jnp.zeros_like(fold)
    stw[0] = jnp.zeros((8, 128), F32)
    sth[0] = jnp.zeros((8, 128), F32)
    rout_row = rout_v[...]
    lasts = []
    for s, grad in enumerate((grad_in, grad_out)):
        square = grad * grad + TINY
        wide = jnp.sum(square, axis=0, keepdims=True)
        for i, part in enumerate(thirds(wide)):
            stw[0, 3 * s + i : 3 * s + i + 1, :] = part
        w0, w1, w2 = thirds(wide)
        lasts.append(((1.0 - DECAY) / (D * FF)) * (w0 + w1 + w2))
        s0, s1, s2 = thirds(square)
        fold[s, 0:HID, :] = s0 + s1 + s2
        row = jnp.sum(jnp.transpose(fold[s]), axis=0, keepdims=True)
        sth[0, 2 * s : 2 * s + 1, :] = row[:, :128]
        sth[0, 2 * s + 1 : 2 * s + 2, :] = row[:, 128:]
    r0, r1, r2 = thirds(rin_v[...])
    stw[0, 6:7, :] = lasts[0] + (DECAY / (64 * D)) * (r0 + r1 + r2)
    lane = lax.broadcasted_iota(jnp.int32, (1, 128), 1)
    tail = jnp.concatenate([rout_row[:, 128:], rout_row[:, 128:]], axis=1)
    tail = jnp.where(lane < 64, tail, 0.0)
    stw[0, 7:8, :] = lasts[1] + (DECAY / (16 * FF)) * (rout_row[:, :128] + tail)

    m0 = remote(stw.at[0], wr0, t0s, t0r, partner)
    m0.start()
    h1 = [remote(sth.at[0], hr1.at[k - 1], u1s.at[k - 1], u1r.at[k - 1], at(x, y + k, z, c)) for k in range(1, 8)]
    for m in h1:
        m.start()
    m0.wait_recv()
    w1 = stw[0] + wr0[...]
    stw[1] = w1
    z1 = [remote(stw.at[1], wr1.at[k - 1], t1s.at[k - 1], t1r.at[k - 1], at(x, y, z + k, c)) for k in range(1, 8)]
    for m in z1:
        m.start()

    part = qown[...]
    for k in (1, 2, 3):
        a1_msg(k).wait_recv()
        part = part + a1r[k - 1].astype(F32)
    a2s[...] = jnp.transpose(part).astype(BF).reshape(8, OUTC, TOK)

    h_sum = sth[0]
    for k, m in enumerate(h1):
        m.wait_recv()
        h_sum = h_sum + hr1[k]
    sth[1] = h_sum
    h2 = remote(sth.at[1], hr2, u2s, u2r, at(x + 4, y, z, c))
    h2.start()
    for k, m in enumerate(z1):
        m.wait_recv()
        w1 = w1 + wr1[k]
    stw[2] = w1
    x2 = [remote(stw.at[2], wr2.at[k - 1], t2s.at[k - 1], t2r.at[k - 1], at(x + k, y, z, c)) for k in range(1, 8)]
    for m in x2:
        m.start()

    def a2_dest(b):
        return 4 * c + b // 2, b % 2

    for b in range(8):
        zz, cc = a2_dest(b)
        mine = jnp.logical_and(zz == z, cc == c)

        @pl.when(mine)
        def _():
            pltpu.make_async_copy(a2s.at[b], a2r.at[z], a2rs.at[z]).start()

        @pl.when(jnp.logical_not(mine))
        def _():
            remote(a2s.at[b], a2r.at[z], a2ss.at[b], a2rs.at[z], at(x, y, zz, cc)).start()

    w_mp = w1
    w_all = w1
    for k, m in enumerate(x2, start=1):
        m.wait_recv()
        got = wr2[k - 1]
        same = ((x - k + 8) % 8) // 4 == h
        w_mp = w_mp + jnp.where(same, got, 0.0)
        w_all = w_all + got
    stw[3] = w_all
    y3 = [remote(stw.at[3], tr3.at[k - 1], t3s.at[k - 1], t3r.at[k - 1], at(x, y + k, z, c)) for k in range(1, 8)]
    for m in y3:
        m.start()
    h2.wait_recv()
    h_sum = h_sum + hr2[...]

    def lanes(t, first):
        return jnp.concatenate([t[first + i : first + i + 1, :] for i in range(3)], axis=1)

    def column(row):
        fold[0, 0:128, :] = jnp.broadcast_to(row[:, :128], (128, 128))
        fold[1, 0:128, :] = jnp.broadcast_to(row[:, 128:], (128, 128))
        return jnp.concatenate([jnp.transpose(fold[0, 0:128, :]), jnp.transpose(fold[1, 0:128, :])[:64]], axis=0)

    def hidden_row(t, first):
        return jnp.concatenate([t[first : first + 1, :], t[first + 1 : first + 2, :]], axis=1)

    def padded(v):
        end = jnp.concatenate([v[:, 128:], v[:, 128:]], axis=1)
        return jnp.concatenate([v[:, :128], end], axis=1)

    rows_in = DECAY * rin_v[...] + ((1.0 - DECAY) / FF) * lanes(w_mp, 0)
    cols_out = DECAY * cout_v[...] + ((1.0 - DECAY) / FF) * lanes(w_mp, 3)
    cols_in = DECAY * padded(cin_v[...]) + ((1.0 - DECAY) / D) * hidden_row(h_sum, 0)
    rows_out = DECAY * padded(rout_v[...]) + ((1.0 - DECAY) / D) * hidden_row(h_sum, 2)
    col_in = column(lax.rsqrt(cols_in))
    col_out = column(lax.rsqrt(rows_out))
    scaled_in = grad_in * lax.rsqrt(rows_in) * jnp.concatenate([col_in] * 3, axis=1)
    scaled_out = grad_out * lax.rsqrt(cols_out) * jnp.concatenate([col_out] * 3, axis=1)

    for k in range(8):
        pltpu.make_async_copy(a2r.at[k], a2r.at[k], a2rs.at[k]).wait()
    total = a2r[0].astype(F32)
    for k in range(1, 8):
        total = total + a2r[k].astype(F32)
    ig_out[...] = total.astype(BF)

    for k, m in enumerate(y3):
        m.wait_recv()
        w_all = w_all + tr3[k]
    mean_in = jnp.sum(w_all[6:7, :], axis=1, keepdims=True)
    mean_out = jnp.sum(w_all[7:8, :], axis=1, keepdims=True)
    nmi_out[...] = min_v[...] - scaled_in * (STEP * jnp.sqrt(mean_in))
    nmo_out[...] = mout_v[...] - scaled_out * (STEP * jnp.sqrt(mean_out))

    @pl.when(a != 1)
    def _():
        remote(xg.at[c, a, 0, z], xg.at[c, a, 0, z], s1s.at[0], s1r.at[0], partner).wait_send()

    for idx in range(1, 4):
        remote(xg.at[c, a, idx, z], xg.at[c, a, idx, z], s1s.at[idx], s1r.at[idx], partner).wait_send()
    for k in (1, 2, 3):
        s2_msg(k).wait_send()
        a1_msg(k).wait_send()
    for k in range(4):
        a0_msg(k).wait_send()
        for rel in range(8):
            share(k, rel).wait_send()
    for d in (0, 1):
        for n in range(14):
            z_msg(d, n).wait_send()
            y_msg(d, n).wait_send()
    cross(0).wait_send()
    cross(1).wait_send()
    for m in (m0, h2, *h1, *z1, *x2, *y3):
        m.wait_send()
    for b in range(8):
        zz, cc = a2_dest(b)

        @pl.when(jnp.logical_not(jnp.logical_and(zz == z, cc == c)))
        def _():
            remote(a2s.at[b], a2r.at[b], a2ss.at[b], a2rs.at[b], partner).wait_send()


def body(
    inputs, pre_act, out_grad, w_in, w_out, master_in, master_out, row_in, col_in, row_out, col_out
):
    dma = pltpu.SemaphoreType.DMA
    vm = pltpu.VMEM
    out = pl.pallas_call(
        kernel,
        name="backward_step",
        out_shape=(
            jax.ShapeDtypeStruct((OUTC, TOK), BF),
            jax.ShapeDtypeStruct((HID, COLS), F32),
            jax.ShapeDtypeStruct((HID, COLS), F32),
        ),
        in_specs=[pl.BlockSpec(memory_space=pl.ANY)] * 11,
        out_specs=[pl.BlockSpec(memory_space=pltpu.VMEM)] * 3,
        scratch_shapes=[
            vm((HID, TOK), BF), vm((TOK, D), BF), vm((HID, D), BF), vm((HID, D), BF),
            vm((HID, COLS), F32), vm((HID, COLS), F32),
            vm((1, COLS), F32), vm((1, HID), F32), vm((1, HID), F32), vm((1, COLS), F32),
            vm((2, 4, 4, 8, RT, COLS), BF), vm((2, HID, 2048), BF), vm((TOK, HID), BF),
            vm((TOK, 768), F32), vm((4, TOK, 768), BF), vm((4, TOK, 768), BF),
            vm((3, TOK, 768), BF), vm((3, TOK, 768), BF), vm((8, OUTC, TOK), BF), vm((8, OUTC, TOK), BF),
            vm((2, 256, 128), F32), vm((4, 8, 128), F32), vm((2, 8, 128), F32),
            vm((8, 128), F32), vm((7, 8, 128), F32), vm((7, 8, 128), F32), vm((7, 8, 128), F32),
            vm((8, 128), F32), vm((7, 8, 128), F32),
            dma((10,)), dma((4,)), dma((4,)), dma((3,)), dma((3,)),
            dma((2, 14)), dma((2, 14)), dma((2, 14)), dma((2, 14)), dma((4, 8)), dma((4, 8)), dma((2,)), dma((2,)),
            dma((4,)), dma((4,)), dma((3,)), dma((3,)), dma((8,)), dma((8,)),
            dma, dma, dma((7,)), dma((7,)), dma((7,)), dma((7,)), dma((7,)), dma((7,)), dma, dma,
            dma((7,)), dma((7,)),
        ],
        compiler_params=pltpu.CompilerParams(
            collective_id=0, has_side_effects=True, vmem_limit_bytes=48 * 2**20
        ),
    )(
        inputs, pre_act.T, out_grad, w_in.T, w_out, master_in.T, master_out,
        row_in.reshape(1, COLS), col_in.reshape(1, HID), row_out.reshape(1, HID), col_out.reshape(1, COLS),
    )
    return out[0].T, out[1].T, out[2]


def solution(mesh):
    return jax.shard_map(
        body,
        mesh=mesh,
        in_specs=(
            P("dp", None),
            P("dp", "mp"),
            P("dp", None),
            P(None, "mp"),
            P("mp", None),
            P("dp", "mp"),
            P("mp", "dp"),
            P("dp"),
            P("mp"),
            P("mp"),
            P("dp"),
        ),
        out_specs=(P("dp", "mp"), P("dp", "mp"), P("mp", "dp")),
        check_vma=False,
    )
```

```python
import math

import jax
import jax.numpy as jnp
from jax import lax
from jax.experimental import pallas as pl
from jax.experimental.pallas import tpu as pltpu
from jax.sharding import PartitionSpec as P

MESH = pl.DeviceIdType.MESH
BF = jnp.bfloat16
F32 = jnp.float32
D = 6144
FF = 12288
TOK = 128
COLS = 384
HID = 192
OUTC = 96
RT = 16
PARTS = 4
KP = D // PARTS
DECAY = 0.8
STEP = 0.05
TINY = 1e-30

NEAR = (0, 1, 7, 2)
FAR = (6, 3, 5, 4)
KINDS = ((1, 0), (0, 0), (1, 1), (0, 1))
LAST = ((0, 3), (1, 2))
ORDER = (
    [("a0", 1), ("a0", 2), ("a0", 3), ("a0", 0), ("s1", 0), ("y", 1, 0), ("s1", 1), ("cross", 1), ("y", 1, 1)]
    + [("s2", 2), ("z", 1, 0), ("a1", 1), ("y", 2, 0), ("s2", 3), ("z", 1, 1), ("a1", 2), ("cross", 0)]
    + [("y", 1, 2), ("z", 1, 2), ("a1", 3), ("y", 2, 1), ("z", 2, 0), ("a1", 0), ("y", 3, 0), ("z", 1, 3)]
    + [("y", 1, 3), ("z", 2, 1), ("y", 2, 2), ("z", 2, 2), ("y", 3, 1), ("z", 3, 0), ("y", 4, 0), ("y", 2, 3)]
    + [("z", 2, 3), ("y", 3, 2), ("z", 3, 1), ("z", 3, 2), ("y", 4, 1), ("y", 3, 3), ("z", 4, 0), ("z", 3, 3)]
    + [("y", 4, 2), ("z", 4, 1), ("z", 4, 2), ("y", 4, 3), ("z", 4, 3)]
)


def xor2(a, k):
    return ((a // 2 + k // 2) % 2) * 2 + (a % 2 + k % 2) % 2


def slot(other, dy):
    dy = dy % 8
    half, place = (0, NEAR.index(dy)) if dy in NEAR else (1, FAR.index(dy))
    return ((other * 2 + half) * 4 + place) * TOK


def message(hop, k):
    return (hop - 1) * 4 + k


def kernel(
    x_hbm, pre_hbm, g_hbm, win_hbm, wout_hbm, min_hbm, mout_hbm, rin_hbm, cin_hbm, rout_hbm, cout_hbm,
    ig_out, nmi_out, nmo_out,
    pre_v, g_v, win_v, wout_v, min_v, mout_v, rin_v, cin_v, rout_v, cout_v,
    xg, hp, p_v, qown, a0s, a0r, a1s, a1r, a2s, a2r, fin, fold, stw, sth, sc_r, sx_r, sz_r, sy_r, st_r, sv_r, hy_r, hx_r,
    lsem, psem, s1s, s1r, s2s, s2r, zs, zr, ys, yr, cs, cr, xs, xr,
    a0ss, a0rs, a1ss, a1rs, a2ss, a2rs, fs, fr, sts, str_, bsem,
):
    dp = lax.axis_index("dp")
    mp = lax.axis_index("mp")
    h, y = dp // 8, dp % 8
    a, z, c = mp // 16, (mp // 2) % 8, mp % 2
    x = h * 4 + a
    inner = (a + 1) // 2 % 2
    is_inner = inner == 1
    is_outer = inner == 0

    def at(xx, yy, zz, cc):
        xx, yy, zz = xx % 8, yy % 8, zz % 8
        return ((xx // 4) * 8 + yy, (xx % 4) * 16 + zz * 2 + cc)

    def remote(src, dst, ss, rs, dev):
        return pltpu.make_async_remote_copy(
            src_ref=src, dst_ref=dst, send_sem=ss, recv_sem=rs, device_id=dev, device_id_type=MESH
        )

    def arrived(ref, sem):
        pltpu.make_async_copy(ref, ref, sem).wait()

    partner = at(x, y, z, 1 - c)
    pair = at(h * 4 + xor2(a, 1), y, z, c)
    x_far = (1 - h) * 4 + 3 - a
    first = [pltpu.make_async_copy(pre_hbm, pre_v, lsem.at[0])]
    parts = []
    for i in range(PARTS):
        cut = slice(i * KP, (i + 1) * KP)
        parts.append(pltpu.make_async_copy(g_hbm.at[:, cut], g_v.at[:, cut], psem.at[i]))
        parts.append(pltpu.make_async_copy(wout_hbm.at[:, cut], wout_v.at[:, cut], psem.at[i]))
    for cp in first + parts:
        cp.start()

    barrier = pltpu.get_barrier_semaphore()

    def greet(dev):
        pl.semaphore_signal(barrier, inc=1, device_id=dev, device_id_type=MESH)

    for k in (4, 3, 5, 2, 6, 1, 7):
        greet(at(x + k, y, z, c))
        greet(at(x, y + k, z, c))
        greet(at(x, y, z + k, c))
    greet(partner)

    @pl.when(is_outer)
    def _():
        for k in (4, 3, 5, 2, 6, 1, 7):
            greet(at(x_far, y + k, z, c))

    loads = [
        pltpu.make_async_copy(s, d, lsem.at[i + 1])
        for i, (s, d) in enumerate(
            (
                (win_hbm, win_v), (min_hbm, min_v), (mout_hbm, mout_v),
                (rin_hbm, rin_v), (cin_hbm, cin_v), (rout_hbm, rout_v), (cout_hbm, cout_v),
            )
        )
    ]
    for cp in loads:
        cp.start()

    first[0].wait()
    pre = pre_v[...].astype(F32)
    cumulative = 0.5 * (1.0 + lax.erf(pre * (1.0 / math.sqrt(2.0))))
    density = jnp.exp(-0.5 * pre * pre) * (1.0 / math.sqrt(2.0 * math.pi))
    own = slot(0, 0)
    hp[1, :, own : own + TOK] = (pre * cumulative).astype(BF)
    slope = cumulative + pre * density

    pl.semaphore_wait(barrier, 22 + 7 * (1 - inner))

    def y_msg(d, hop, kind):
        of, other = KINDS[kind]
        sgn = 1 if d == 0 else -1
        n = message(hop, kind) if hop < 4 else 12 + LAST[d].index(kind)
        b, e = slot(other, -sgn * (hop - 1)), slot(other, -sgn * hop)
        return remote(hp.at[of, :, b : b + TOK], hp.at[of, :, e : e + TOK], ys, yr.at[d, n], at(x, y + sgn, z, c))

    def cross(of):
        b, e = slot(0, 0), slot(1, 0)
        return remote(hp.at[of, :, b : b + TOK], hp.at[of, :, e : e + TOK], xs, xr.at[of], at(x + 4, y, z, c))

    cross(1).start()

    set_q = 2 * (1 - inner)

    def s1_start(src):
        def piece(dy):
            y_to = (y - dy) % 8
            half, place = (0, NEAR.index(dy)) if dy in NEAR else (1, FAR.index(dy))
            x_to = jnp.where(is_inner, x, x_far)
            j = (x_to // 4) * 8 + y_to
            there = xg.at[c, set_q + half, place, z]
            cut = src.at[pl.ds(pl.multiple_of(RT * z, RT), RT), pl.ds(pl.multiple_of(COLS * j, COLS), COLS)]
            return cut, there, s1r.at[half], at(x_to, y_to, z, c)

        def one(dy):
            cut, there, sem, dev = piece(dy)
            remote(cut, there, s1s, sem, dev).start()

        @pl.when(is_inner)
        def _():
            cut, there, sem, _ = piece(0)
            pltpu.make_async_copy(cut, there, sem).start()

        @pl.when(is_outer)
        def _():
            one(0)

        for dy in (1, 7, 2, 6, 3, 5, 4):
            one(dy)

    @pl.when(c == 0)
    def _():
        s1_start(x_hbm)

    @pl.when(c == 1)
    def _():
        s1_start(g_hbm)

    for d in (0, 1):
        y_msg(d, 1, 0).start()

    hid_grad = jnp.zeros((HID, TOK), F32)
    for i in range(PARTS):
        cut = slice(i * KP, (i + 1) * KP)
        parts[2 * i].wait()
        parts[2 * i + 1].wait()
        hid_grad += lax.dot_general(wout_v[:, cut], g_v[:, cut], (((1,), (1,)), ((), ())), preferred_element_type=F32)
    pre_grad = hid_grad * slope
    hp[0, :, own : own + TOK] = pre_grad.astype(BF)
    p_v[...] = jnp.transpose(pre_grad).astype(BF)
    cross(0).start()
    for d in (0, 1):
        y_msg(d, 1, 1).start()

    def chunk(k):
        return (set_q + k) % 4

    def piece_of(k, zo):
        return xg.at[c, chunk(k), :, zo % 8]

    def z_msg(d, hop, k):
        sgn = 1 if d == 0 else -1
        n = message(hop, k) if hop < 4 else 12 + LAST[d].index(k)
        ref = piece_of(k, z - sgn * (hop - 1))
        return remote(ref, ref, zs, zr.at[d, n], at(x, y, z + sgn, c))

    def share(k, rel):
        ref = piece_of(k, z + rel)
        return remote(ref, ref, cs, cr.at[k], partner)

    def s2_msg(k):
        ref = piece_of(k, z)
        return remote(ref, ref, s2s, s2r.at[k], pair)

    def product(k, half):
        at_col = pl.multiple_of(1536 * xor2(a, k) + 768 * half, 128)
        return jnp.dot(p_v[...], win_v[:, pl.ds(at_col, 768)], preferred_element_type=F32)

    def a0_msg(k):
        return remote(a0s.at[k], a0r.at[k], a0ss, a0rs.at[k], partner)

    def a1_msg(k):
        return remote(a1s.at[k - 1], a1r.at[k - 1], a1ss, a1rs, at(h * 4 + xor2(a, k), y, z, c))

    loads[0].wait()
    for event in ORDER:
        what, *rest = event
        if what == "s1":
            (k,) = rest
            arrived(piece_of(k, z), s1r.at[k])
            s2_msg(k).start()
            for d in (0, 1):
                z_msg(d, 1, k).start()
            share(k, 0).start()
        elif what == "s2":
            (k,) = rest
            s2_msg(k - 2).wait_recv()
            for d in (0, 1):
                z_msg(d, 1, k).start()
            share(k, 0).start()
        elif what == "cross":
            (of,) = rest
            cross(of).wait_recv()
            for d in (0, 1):
                y_msg(d, 1, 2 if of == 1 else 3).start()
        elif what in ("y", "z"):
            hop, k = rest
            make = y_msg if what == "y" else z_msg
            for d in (0, 1):
                sgn = 1 if d == 0 else -1
                if hop == 4 and k not in LAST[d]:
                    continue
                make(d, hop, k).wait_recv()
                if hop < 3 or (hop == 3 and k in LAST[d]):
                    make(d, hop + 1, k).start()
                if what == "z":
                    share(k, -sgn * hop).start()
        elif what == "a0":
            (k,) = rest
            a0s[k] = product(k, 1 - c).astype(BF)
            a0_msg(k).start()
        elif what == "a1":
            (k,) = rest
            mine = product(k, c)
            a0_msg(k).wait_recv()
            mine = mine + a0r[k].astype(F32)
            if k:
                a1s[k - 1] = mine.astype(BF)
                a1_msg(k).start()
            else:
                qown[...] = mine
    for k in range(4):
        arrived(xg.at[1 - c, chunk(k)], cr.at[k])

    def gradient(of):
        total = jnp.zeros((HID, COLS), F32)
        for q in range(4):
            total += jnp.dot(
                hp[of, :, 512 * q : 512 * (q + 1)], xg[of, q].reshape(512, COLS), preferred_element_type=F32
            )
        return total

    grad_in = gradient(0)
    grad_out = gradient(1)

    def thirds(v):
        return v[:, :128], v[:, 128:256], v[:, 256:]

    for cp in loads[1:]:
        cp.wait()
    fold[...] = jnp.zeros_like(fold)
    sth[0] = jnp.zeros((8, 128), F32)
    rout_row = rout_v[...]
    lasts = []
    for s, grad in enumerate((grad_in, grad_out)):
        square = grad * grad + TINY
        wide = jnp.sum(square, axis=0, keepdims=True)
        w0, w1, w2 = thirds(wide)
        for i, part in enumerate((w0, w1, w2)):
            stw[0, 3 * s + i : 3 * s + i + 1, :] = part
        lasts.append(((1.0 - DECAY) / (D * FF)) * (w0 + w1 + w2))
        s0, s1, s2 = thirds(square)
        fold[s, 0:HID, :] = s0 + s1 + s2
        row = jnp.sum(jnp.transpose(fold[s]), axis=0, keepdims=True)
        sth[0, 2 * s : 2 * s + 1, :] = row[:, :128]
        sth[0, 2 * s + 1 : 2 * s + 2, :] = row[:, 128:]
    r0, r1, r2 = thirds(rin_v[...].reshape(1, COLS))
    stw[0, 6:7, :] = lasts[0] + (DECAY / (64 * D)) * (r0 + r1 + r2)
    lane = lax.broadcasted_iota(jnp.int32, (1, 128), 1)
    tail = jnp.concatenate([rout_row[:, 128:], rout_row[:, 128:]], axis=1)
    tail = jnp.where(lane < 64, tail, 0.0)
    stw[0, 7:8, :] = lasts[1] + (DECAY / (16 * FF)) * (rout_row[:, :128] + tail)

    def ring_of(axis, k):
        return at(x + k * (axis == "x"), y + k * (axis == "y"), z + k * (axis == "z"), c)

    def spread(src, dst, i, axis):
        ms = [remote(src, dst.at[k - 1], sts, str_.at[i], ring_of(axis, k)) for k in (4, 3, 5, 2, 6, 1, 7)]
        for m in ms:
            m.start()

    m0 = remote(stw.at[0], sc_r, sts, str_.at[0], partner)
    m0.start()
    spread(sth.at[0], hy_r, 1, "y")
    m0.wait_recv()
    w_sum = stw[0] + sc_r[...]
    stw[1] = w_sum
    spread(stw.at[1], sx_r, 2, "x")

    arrived(a1r, a1rs)
    part = qown[...]
    for k in range(3):
        part = part + a1r[k].astype(F32)
    a2s[...] = jnp.transpose(part).astype(BF).reshape(4, 2 * OUTC, TOK)

    arrived(hy_r, str_.at[1])
    h_sum = sth[0]
    for k in range(7):
        h_sum = h_sum + hy_r[k]
    sth[1] = h_sum
    hx = remote(sth.at[1], hx_r, sts, str_.at[3], at(x + 4, y, z, c))
    hx.start()

    arrived(sx_r, str_.at[2])
    w_mp = w_sum
    t_sum = w_sum
    for k in range(1, 8):
        got = sx_r[k - 1]
        same = ((x - k + 8) % 8) // 4 == h
        w_mp = w_mp + jnp.where(same, got, 0.0)
        t_sum = t_sum + got
    stw[2] = t_sum
    spread(stw.at[2, pl.ds(6, 2)], sy_r, 4, "y")
    stw[3] = w_mp
    spread(stw.at[3], sz_r, 5, "z")

    for b in range(4):
        zz = 4 * c + b

        @pl.when(zz == z)
        def _():
            pltpu.make_async_copy(a2s.at[b], a2r.at[z], a2rs).start()

        @pl.when(zz != z)
        def _():
            remote(a2s.at[b], a2r.at[z], a2ss, a2rs, at(x, y, zz, c)).start()

    arrived(sy_r, str_.at[4])
    t_two = t_sum[6:8, :]
    for k in range(7):
        t_two = t_two + sy_r[k]
    st_r[7] = t_two
    spread(st_r.at[7], sv_r, 6, "z")

    arrived(sz_r, str_.at[5])
    for k in range(7):
        w_mp = w_mp + sz_r[k]
    hx.wait_recv()
    h_sum = h_sum + hx_r[...]

    def lanes(t, first_row):
        return jnp.concatenate([t[first_row + i : first_row + i + 1, :] for i in range(3)], axis=1)

    def column(row):
        fold[0, 0:128, :] = jnp.broadcast_to(row[:, :128], (128, 128))
        fold[1, 0:128, :] = jnp.broadcast_to(row[:, 128:], (128, 128))
        return jnp.concatenate([jnp.transpose(fold[0, 0:128, :]), jnp.transpose(fold[1, 0:128, :])[:64]], axis=0)

    def hidden_row(t, first_row):
        return jnp.concatenate([t[first_row : first_row + 1, :], t[first_row + 1 : first_row + 2, :]], axis=1)

    def padded(v):
        end = jnp.concatenate([v[:, 128:], v[:, 128:]], axis=1)
        return jnp.concatenate([v[:, :128], end], axis=1)

    rows_in = DECAY * rin_v[...].reshape(1, COLS) + ((1.0 - DECAY) / FF) * lanes(w_mp, 0)
    cols_out = DECAY * cout_v[...].reshape(1, COLS) + ((1.0 - DECAY) / FF) * lanes(w_mp, 3)
    cols_in = DECAY * padded(cin_v[...]) + ((1.0 - DECAY) / D) * hidden_row(h_sum, 0)
    rows_out = DECAY * padded(rout_v[...]) + ((1.0 - DECAY) / D) * hidden_row(h_sum, 2)
    col_in = column(lax.rsqrt(cols_in))
    col_out = column(lax.rsqrt(rows_out))
    scaled_in = grad_in * lax.rsqrt(rows_in) * jnp.concatenate([col_in] * 3, axis=1)
    scaled_out = grad_out * lax.rsqrt(cols_out) * jnp.concatenate([col_out] * 3, axis=1)

    collects = z // 4 == c

    def last_msg():
        return remote(fin, ig_out, fs, fr, partner)

    @pl.when(collects)
    def _():
        arrived(a2r, a2rs)
        total = a2r[0].astype(F32)
        for k in range(1, 8):
            total = total + a2r[k].astype(F32)
        upper, lower = total[:OUTC].astype(BF), total[OUTC:].astype(BF)

        @pl.when(c == 0)
        def _():
            ig_out[...] = upper
            fin[...] = lower

        @pl.when(c == 1)
        def _():
            ig_out[...] = lower
            fin[...] = upper

        last_msg().start()
        last_msg().wait_send()

    @pl.when(jnp.logical_not(collects))
    def _():
        last_msg().wait_recv()

    @pl.when(is_inner)
    def _():
        arrived(xg.at[c, 0, 0, 0:7], s1s)

    @pl.when(is_outer)
    def _():
        arrived(xg.at[c, 0, 0], s1s)

    arrived(xg.at[c, 0:2, :, 0], s2s)
    arrived(a0s, a0ss)
    arrived(a1s, a1ss)
    arrived(xg.at[c], cs)
    arrived(xg.at[c, :, :, 0:7], zs)
    arrived(hp.at[:, :, 0:1792], ys)
    arrived(hp.at[:, :, 0:TOK], xs)

    @pl.when(collects)
    def _():
        arrived(a2s.at[0:3], a2ss)

    @pl.when(jnp.logical_not(collects))
    def _():
        arrived(a2s, a2ss)

    arrived(sv_r, str_.at[6])
    for k in range(7):
        t_two = t_two + sv_r[k]
    mean_in = jnp.sum(t_two[0:1, :], axis=1, keepdims=True)
    mean_out = jnp.sum(t_two[1:2, :], axis=1, keepdims=True)
    nmi_out[...] = min_v[...] - scaled_in * (STEP * jnp.sqrt(mean_in))
    nmo_out[...] = mout_v[...] - scaled_out * (STEP * jnp.sqrt(mean_out))
    for ref in (stw.at[0], hy_r, sx_r, hx_r, sz_r):
        arrived(ref, sts)
    arrived(sy_r, sts)
    arrived(sv_r, sts)


def put_out(ig, nmi, nmo, ig_out, nmi_out, nmo_out, sem):
    copies = [
        pltpu.make_async_copy(s, d, sem.at[i]) for i, (s, d) in enumerate(((nmi, nmi_out), (nmo, nmo_out), (ig, ig_out)))
    ]
    for cp in copies:
        cp.start()
    for cp in copies:
        cp.wait()


def body(
    inputs, pre_act, out_grad, w_in, w_out, master_in, master_out, row_in, col_in, row_out, col_out
):
    dma = pltpu.SemaphoreType.DMA
    vm = pltpu.VMEM
    shapes = (
        jax.ShapeDtypeStruct((OUTC, TOK), BF),
        jax.ShapeDtypeStruct((HID, COLS), F32),
        jax.ShapeDtypeStruct((HID, COLS), F32),
    )
    made = pl.pallas_call(
        kernel,
        name="backward_step",
        out_shape=shapes,
        in_specs=[pl.BlockSpec(memory_space=pl.ANY)] * 11,
        out_specs=[pl.BlockSpec(memory_space=pltpu.VMEM)] * 3,
        scratch_shapes=[
            vm((HID, TOK), BF), vm((TOK, D), BF), vm((HID, D), BF), vm((HID, D), BF),
            vm((HID, COLS), F32), vm((HID, COLS), F32),
            vm((COLS,), F32), vm((1, HID), F32), vm((1, HID), F32), vm((COLS,), F32),
            vm((2, 4, 4, 8, RT, COLS), BF), vm((2, HID, 2048), BF), vm((TOK, HID), BF),
            vm((TOK, 768), F32), vm((4, TOK, 768), BF), vm((4, TOK, 768), BF),
            vm((3, TOK, 768), BF), vm((3, TOK, 768), BF), vm((4, 2 * OUTC, TOK), BF), vm((8, 2 * OUTC, TOK), BF),
            vm((OUTC, TOK), BF),
            vm((2, 256, 128), F32), vm((4, 8, 128), F32), vm((2, 8, 128), F32),
            vm((8, 128), F32), vm((7, 8, 128), F32), vm((7, 8, 128), F32), vm((7, 2, 128), F32),
            vm((8, 2, 128), F32), vm((7, 2, 128), F32), vm((7, 8, 128), F32), vm((8, 128), F32),
            dma((8,)), dma((PARTS,)), dma, dma((2,)), dma, dma((2,)),
            dma, dma((2, 14)), dma, dma((2, 14)), dma, dma((4,)), dma, dma((2,)),
            dma, dma((4,)), dma, dma, dma, dma, dma, dma, dma, dma((7,)), dma,
        ],
        compiler_params=pltpu.CompilerParams(
            collective_id=0, has_side_effects=True, vmem_limit_bytes=48 * 2**20
        ),
    )(
        *(
            pltpu.with_memory_space_constraint(v, pltpu.HBM)
            for v in (
                inputs, pre_act.T, out_grad, w_in.T, w_out, master_in.T, master_out,
                row_in, col_in.reshape(1, HID), row_out.reshape(1, HID), col_out,
            )
        )
    )
    out = pl.pallas_call(
        put_out,
        name="put_out",
        out_shape=shapes,
        in_specs=[pl.BlockSpec(memory_space=pl.ANY)] * 3,
        out_specs=[pl.BlockSpec(memory_space=pl.ANY)] * 3,
        scratch_shapes=[dma((3,))],
        compiler_params=pltpu.CompilerParams(vmem_limit_bytes=2**20),
    )(*made)
    return out[0].T, out[1].T, out[2]


def solution(mesh):
    return jax.shard_map(
        body,
        mesh=mesh,
        in_specs=(
            P("dp", None),
            P("dp", "mp"),
            P("dp", None),
            P(None, "mp"),
            P("mp", None),
            P("dp", "mp"),
            P("mp", "dp"),
            P("dp"),
            P("mp"),
            P("mp"),
            P("dp"),
        ),
        out_specs=(P("dp", "mp"), P("dp", "mp"), P("mp", "dp")),
        check_vma=False,
    )
```

```python
import math

import jax
import jax.numpy as jnp
from jax import lax
from jax.experimental import pallas as pl
from jax.experimental.pallas import tpu as pltpu
from jax.sharding import PartitionSpec as P

MESH = pl.DeviceIdType.MESH
BF = jnp.bfloat16
F32 = jnp.float32
D = 6144
FF = 12288
TOK = 128
COLS = 384
HID = 192
OUTC = 96
RT = 16
PARTS = 4
KP = D // PARTS
DECAY = 0.8
STEP = 0.05
TINY = 1e-30

NEAR = (0, 1, 7, 2)
FAR = (6, 3, 5, 4)
KINDS = ((1, 0), (0, 0), (1, 1), (0, 1))
LAST = ((0, 3), (1, 2))
ORDER = (
    [("a0", 1), ("a0", 2), ("a0", 3), ("a0", 0), ("y", 1, 0), ("s1", 0), ("cross", 1), ("y", 1, 1), ("s1", 1)]
    + [("cross", 0), ("y", 2, 0), ("a1", 1), ("s2", 2), ("y", 1, 2), ("z", 1, 0), ("a1", 2), ("y", 2, 1), ("s2", 3)]
    + [("z", 1, 1), ("y", 1, 3), ("a1", 3), ("y", 3, 0), ("z", 1, 2), ("y", 2, 2), ("a1", 0), ("z", 2, 0)]
    + [("z", 1, 3), ("y", 3, 1), ("z", 2, 1), ("y", 2, 3), ("z", 2, 2), ("y", 4, 0), ("y", 3, 2), ("z", 3, 0)]
    + [("z", 2, 3), ("y", 4, 1), ("y", 3, 3), ("z", 3, 1), ("z", 3, 2), ("y", 4, 2), ("z", 4, 0), ("z", 3, 3)]
    + [("y", 4, 3), ("z", 4, 1), ("z", 4, 2), ("z", 4, 3)]
)


def xor2(a, k):
    return ((a // 2 + k // 2) % 2) * 2 + (a % 2 + k % 2) % 2


def slot(other, dy):
    dy = dy % 8
    half, place = (0, NEAR.index(dy)) if dy in NEAR else (1, FAR.index(dy))
    return ((other * 2 + half) * 4 + place) * TOK


def message(hop, k):
    return (hop - 1) * 4 + k


def kernel(
    x_hbm, pre_hbm, g_hbm, win_hbm, wout_hbm, min_hbm, mout_hbm, rin_hbm, cin_hbm, rout_hbm, cout_hbm,
    ig_out, nmi_out, nmo_out,
    pre_v, g_v, win_v, wout_v, min_v, mout_v, rin_v, cin_v, rout_v, cout_v,
    xg, hp, p_v, qown, a0s, a0r, a1s, a1r, a2s, a2r, fin, src_v, fold, stw, sth, sc_r, sx_r, sz_r, sy_r, st_r, sv_r, hy_r, hx_r,
    lsem, psem, s1s, s1r, s2s, s2r, zs, zr, ys, yr, cs, cr, xs, xr,
    a0ss, a0rs, a1ss, a1rs, a2ss, a2rs, fs, fr, sts, str_, bsem,
):
    dp = lax.axis_index("dp")
    mp = lax.axis_index("mp")
    h, y = dp // 8, dp % 8
    a, z, c = mp // 16, (mp // 2) % 8, mp % 2
    x = h * 4 + a
    inner = (a + 1) // 2 % 2
    is_inner = inner == 1
    is_outer = inner == 0

    def at(xx, yy, zz, cc):
        xx, yy, zz = xx % 8, yy % 8, zz % 8
        return ((xx // 4) * 8 + yy, (xx % 4) * 16 + zz * 2 + cc)

    def remote(src, dst, ss, rs, dev):
        return pltpu.make_async_remote_copy(
            src_ref=src, dst_ref=dst, send_sem=ss, recv_sem=rs, device_id=dev, device_id_type=MESH
        )

    def arrived(ref, sem):
        pltpu.make_async_copy(ref, ref, sem).wait()

    partner = at(x, y, z, 1 - c)
    pair = at(h * 4 + xor2(a, 1), y, z, c)
    x_far = (1 - h) * 4 + 3 - a
    first = [pltpu.make_async_copy(pre_hbm, pre_v, lsem.at[0])]
    parts = []
    for i in range(PARTS):
        cut = slice(i * KP, (i + 1) * KP)
        parts.append(pltpu.make_async_copy(g_hbm.at[:, cut], g_v.at[:, cut], psem.at[i]))
        parts.append(pltpu.make_async_copy(wout_hbm.at[:, cut], wout_v.at[:, cut], psem.at[i]))
    rows = pl.ds(pl.multiple_of(RT * z, RT), RT)

    @pl.when(c == 0)
    def _():
        pltpu.make_async_copy(x_hbm.at[rows], src_v, bsem).start()

    @pl.when(c == 1)
    def _():
        pltpu.make_async_copy(g_hbm.at[rows], src_v, bsem).start()

    for cp in first + parts:
        cp.start()

    barrier = pltpu.get_barrier_semaphore()

    def greet(dev):
        pl.semaphore_signal(barrier, inc=1, device_id=dev, device_id_type=MESH)

    for k in (4, 3, 5, 2, 6, 1, 7):
        greet(at(x + k, y, z, c))
        greet(at(x, y + k, z, c))
    greet(at(x, y, z + 1, c))
    greet(at(x, y, z + 7, c))
    greet(partner)

    @pl.when(is_outer)
    def _():
        for k in (4, 3, 5, 2, 6, 1, 7):
            greet(at(x_far, y + k, z, c))

    loads = [
        pltpu.make_async_copy(s, d, lsem.at[i + 1])
        for i, (s, d) in enumerate(
            (
                (win_hbm, win_v), (min_hbm, min_v), (mout_hbm, mout_v),
                (rin_hbm, rin_v), (cin_hbm, cin_v), (rout_hbm, rout_v), (cout_hbm, cout_v),
            )
        )
    ]
    for cp in loads:
        cp.start()

    first[0].wait()
    pre = pre_v[...].astype(F32)
    cumulative = 0.5 * (1.0 + lax.erf(pre * (1.0 / math.sqrt(2.0))))
    density = jnp.exp(-0.5 * pre * pre) * (1.0 / math.sqrt(2.0 * math.pi))
    own = slot(0, 0)
    hp[1, :, own : own + TOK] = (pre * cumulative).astype(BF)
    slope = cumulative + pre * density

    pl.semaphore_wait(barrier, 17 + 7 * (1 - inner))

    def y_msg(d, hop, kind):
        of, other = KINDS[kind]
        sgn = 1 if d == 0 else -1
        n = message(hop, kind) if hop < 4 else 12 + LAST[d].index(kind)
        b, e = slot(other, -sgn * (hop - 1)), slot(other, -sgn * hop)
        return remote(hp.at[of, :, b : b + TOK], hp.at[of, :, e : e + TOK], ys, yr.at[d, n], at(x, y + sgn, z, c))

    def cross(of):
        b, e = slot(0, 0), slot(1, 0)
        return remote(hp.at[of, :, b : b + TOK], hp.at[of, :, e : e + TOK], xs, xr.at[of], at(x + 4, y, z, c))

    cross(1).start()

    set_q = 2 * (1 - inner)

    def piece(dy):
        y_to = (y - dy) % 8
        half, place = (0, NEAR.index(dy)) if dy in NEAR else (1, FAR.index(dy))
        x_to = jnp.where(is_inner, x, x_far)
        j = (x_to // 4) * 8 + y_to
        there = xg.at[c, set_q + half, place, z]
        return src_v.at[:, pl.ds(pl.multiple_of(COLS * j, COLS), COLS)], there, s1r.at[half], at(x_to, y_to, z, c)

    def one(dy):
        cut, there, sem, dev = piece(dy)
        remote(cut, there, s1s, sem, dev).start()

    arrived(src_v, bsem)

    @pl.when(is_inner)
    def _():
        cut, there, sem, _ = piece(0)
        pltpu.make_async_copy(cut, there, sem).start()

    @pl.when(is_outer)
    def _():
        one(0)

    for dy in (1, 7, 2, 6, 3, 5, 4):
        one(dy)

    for d in (0, 1):
        y_msg(d, 1, 0).start()

    hid_grad = jnp.zeros((HID, TOK), F32)
    for i in range(PARTS):
        cut = slice(i * KP, (i + 1) * KP)
        parts[2 * i].wait()
        parts[2 * i + 1].wait()
        hid_grad += lax.dot_general(wout_v[:, cut], g_v[:, cut], (((1,), (1,)), ((), ())), preferred_element_type=F32)
    pre_grad = hid_grad * slope
    hp[0, :, own : own + TOK] = pre_grad.astype(BF)
    p_v[...] = jnp.transpose(pre_grad).astype(BF)
    cross(0).start()
    for d in (0, 1):
        y_msg(d, 1, 1).start()

    def chunk(k):
        return (set_q + k) % 4

    def piece_of(k, zo):
        return xg.at[c, chunk(k), :, zo % 8]

    def z_msg(d, hop, k):
        sgn = 1 if d == 0 else -1
        n = message(hop, k) if hop < 4 else 12 + LAST[d].index(k)
        ref = piece_of(k, z - sgn * (hop - 1))
        return remote(ref, ref, zs, zr.at[d, n], at(x, y, z + sgn, c))

    def share(k, rel):
        ref = piece_of(k, z + rel)
        return remote(ref, ref, cs, cr.at[k], partner)

    def s2_msg(k):
        ref = piece_of(k, z)
        return remote(ref, ref, s2s, s2r.at[k], pair)

    def product(k, half):
        at_col = pl.multiple_of(1536 * xor2(a, k) + 768 * half, 128)
        return jnp.dot(p_v[...], win_v[:, pl.ds(at_col, 768)], preferred_element_type=F32)

    def a0_msg(k):
        return remote(a0s.at[k], a0r.at[k], a0ss, a0rs.at[k], partner)

    def a1_msg(k):
        return remote(a1s.at[k - 1], a1r.at[k - 1], a1ss, a1rs, at(h * 4 + xor2(a, k), y, z, c))

    loads[0].wait()
    for event in ORDER:
        what, *rest = event
        if what == "s1":
            (k,) = rest
            arrived(piece_of(k, z), s1r.at[k])
            s2_msg(k).start()
            for d in (0, 1):
                z_msg(d, 1, k).start()
            share(k, 0).start()
        elif what == "s2":
            (k,) = rest
            s2_msg(k - 2).wait_recv()
            for d in (0, 1):
                z_msg(d, 1, k).start()
            share(k, 0).start()
        elif what == "cross":
            (of,) = rest
            cross(of).wait_recv()
            for d in (0, 1):
                y_msg(d, 1, 2 if of == 1 else 3).start()
        elif what in ("y", "z"):
            hop, k = rest
            make = y_msg if what == "y" else z_msg
            for d in (0, 1):
                sgn = 1 if d == 0 else -1
                if hop == 4 and k not in LAST[d]:
                    continue
                make(d, hop, k).wait_recv()
                if hop < 3 or (hop == 3 and k in LAST[d]):
                    make(d, hop + 1, k).start()
                if what == "z":
                    share(k, -sgn * hop).start()
        elif what == "a0":
            (k,) = rest
            a0s[k] = product(k, 1 - c).astype(BF)
            a0_msg(k).start()
        elif what == "a1":
            (k,) = rest
            mine = product(k, c)
            a0_msg(k).wait_recv()
            mine = mine + a0r[k].astype(F32)
            if k:
                a1s[k - 1] = mine.astype(BF)
                a1_msg(k).start()
            else:
                qown[...] = mine
    for k in range(4):
        arrived(xg.at[1 - c, chunk(k)], cr.at[k])

    def gradient(of):
        total = jnp.zeros((HID, COLS), F32)
        for q in range(4):
            total += jnp.dot(
                hp[of, :, 512 * q : 512 * (q + 1)], xg[of, q].reshape(512, COLS), preferred_element_type=F32
            )
        return total

    grad_in = gradient(0)
    grad_out = gradient(1)

    def thirds(v):
        return v[:, :128], v[:, 128:256], v[:, 256:]

    for cp in loads[1:]:
        cp.wait()
    fold[...] = jnp.zeros_like(fold)
    sth[0] = jnp.zeros((8, 128), F32)
    rout_row = rout_v[...]
    lasts = []
    for s, grad in enumerate((grad_in, grad_out)):
        square = grad * grad + TINY
        wide = jnp.sum(square, axis=0, keepdims=True)
        w0, w1, w2 = thirds(wide)
        for i, part in enumerate((w0, w1, w2)):
            stw[0, 3 * s + i : 3 * s + i + 1, :] = part
        lasts.append(((1.0 - DECAY) / (D * FF)) * (w0 + w1 + w2))
        s0, s1, s2 = thirds(square)
        fold[s, 0:HID, :] = s0 + s1 + s2
        row = jnp.sum(jnp.transpose(fold[s]), axis=0, keepdims=True)
        sth[0, 2 * s : 2 * s + 1, :] = row[:, :128]
        sth[0, 2 * s + 1 : 2 * s + 2, :] = row[:, 128:]
    r0, r1, r2 = thirds(rin_v[...].reshape(1, COLS))
    stw[0, 6:7, :] = lasts[0] + (DECAY / (64 * D)) * (r0 + r1 + r2)
    lane = lax.broadcasted_iota(jnp.int32, (1, 128), 1)
    tail = jnp.concatenate([rout_row[:, 128:], rout_row[:, 128:]], axis=1)
    tail = jnp.where(lane < 64, tail, 0.0)
    stw[0, 7:8, :] = lasts[1] + (DECAY / (16 * FF)) * (rout_row[:, :128] + tail)

    def ring_of(axis, k):
        return at(x + k * (axis == "x"), y + k * (axis == "y"), z + k * (axis == "z"), c)

    def spread(src, dst, i, axis):
        ms = [remote(src, dst.at[k - 1], sts, str_.at[i], ring_of(axis, k)) for k in (4, 3, 5, 2, 6, 1, 7)]
        for m in ms:
            m.start()

    m0 = remote(stw.at[0], sc_r, sts, str_.at[0], partner)
    m0.start()
    spread(sth.at[0], hy_r, 1, "y")
    m0.wait_recv()
    w_sum = stw[0] + sc_r[...]
    stw[1] = w_sum
    spread(stw.at[1], sx_r, 2, "x")

    arrived(a1r, a1rs)
    part = qown[...]
    for k in range(3):
        part = part + a1r[k].astype(F32)
    a2s[...] = jnp.transpose(part).astype(BF).reshape(4, 2 * OUTC, TOK)
    for b in range(4):
        zz = 4 * c + b

        @pl.when(zz == z)
        def _():
            pltpu.make_async_copy(a2s.at[b], a2r.at[z], a2rs).start()

        @pl.when(zz != z)
        def _():
            remote(a2s.at[b], a2r.at[z], a2ss, a2rs, at(x, y, zz, c)).start()

    arrived(hy_r, str_.at[1])
    h_sum = sth[0]
    for k in range(7):
        h_sum = h_sum + hy_r[k]
    sth[1] = h_sum
    hx = remote(sth.at[1], hx_r, sts, str_.at[3], at(x + 4, y, z, c))
    hx.start()

    arrived(sx_r, str_.at[2])
    w_mp = w_sum
    t_sum = w_sum
    for k in range(1, 8):
        got = sx_r[k - 1]
        same = ((x - k + 8) % 8) // 4 == h
        w_mp = w_mp + jnp.where(same, got, 0.0)
        t_sum = t_sum + got
    stw[2] = t_sum
    spread(stw.at[2, pl.ds(6, 2)], sy_r, 4, "y")
    stw[3] = w_mp
    spread(stw.at[3], sz_r, 5, "z")

    arrived(sy_r, str_.at[4])
    t_two = t_sum[6:8, :]
    for k in range(7):
        t_two = t_two + sy_r[k]
    st_r[7] = t_two
    spread(st_r.at[7], sv_r, 6, "z")

    arrived(sz_r, str_.at[5])
    for k in range(7):
        w_mp = w_mp + sz_r[k]
    hx.wait_recv()
    h_sum = h_sum + hx_r[...]

    def lanes(t, first_row):
        return jnp.concatenate([t[first_row + i : first_row + i + 1, :] for i in range(3)], axis=1)

    def column(row):
        fold[0, 0:128, :] = jnp.broadcast_to(row[:, :128], (128, 128))
        fold[1, 0:128, :] = jnp.broadcast_to(row[:, 128:], (128, 128))
        return jnp.concatenate([jnp.transpose(fold[0, 0:128, :]), jnp.transpose(fold[1, 0:128, :])[:64]], axis=0)

    def hidden_row(t, first_row):
        return jnp.concatenate([t[first_row : first_row + 1, :], t[first_row + 1 : first_row + 2, :]], axis=1)

    def padded(v):
        end = jnp.concatenate([v[:, 128:], v[:, 128:]], axis=1)
        return jnp.concatenate([v[:, :128], end], axis=1)

    rows_in = DECAY * rin_v[...].reshape(1, COLS) + ((1.0 - DECAY) / FF) * lanes(w_mp, 0)
    cols_out = DECAY * cout_v[...].reshape(1, COLS) + ((1.0 - DECAY) / FF) * lanes(w_mp, 3)
    cols_in = DECAY * padded(cin_v[...]) + ((1.0 - DECAY) / D) * hidden_row(h_sum, 0)
    rows_out = DECAY * padded(rout_v[...]) + ((1.0 - DECAY) / D) * hidden_row(h_sum, 2)
    col_in = column(lax.rsqrt(cols_in))
    col_out = column(lax.rsqrt(rows_out))
    scaled_in = grad_in * lax.rsqrt(rows_in) * jnp.concatenate([col_in] * 3, axis=1)
    scaled_out = grad_out * lax.rsqrt(cols_out) * jnp.concatenate([col_out] * 3, axis=1)

    collects = z // 4 == c

    def last_msg():
        return remote(fin, ig_out, fs, fr, partner)

    @pl.when(collects)
    def _():
        arrived(a2r, a2rs)
        total = a2r[0].astype(F32)
        for k in range(1, 8):
            total = total + a2r[k].astype(F32)
        upper, lower = total[:OUTC].astype(BF), total[OUTC:].astype(BF)

        @pl.when(c == 0)
        def _():
            ig_out[...] = upper
            fin[...] = lower

        @pl.when(c == 1)
        def _():
            ig_out[...] = lower
            fin[...] = upper

        last_msg().start()
        last_msg().wait_send()

    @pl.when(jnp.logical_not(collects))
    def _():
        last_msg().wait_recv()

    @pl.when(is_inner)
    def _():
        arrived(xg.at[c, 0, 0, 0:7], s1s)

    @pl.when(is_outer)
    def _():
        arrived(xg.at[c, 0, 0], s1s)

    arrived(xg.at[c, 0:2, :, 0], s2s)
    arrived(a0s, a0ss)
    arrived(a1s, a1ss)
    arrived(xg.at[c], cs)
    arrived(xg.at[c, :, :, 0:7], zs)
    arrived(hp.at[:, :, 0:1792], ys)
    arrived(hp.at[:, :, 0:TOK], xs)

    @pl.when(collects)
    def _():
        arrived(a2s.at[0:3], a2ss)

    @pl.when(jnp.logical_not(collects))
    def _():
        arrived(a2s, a2ss)

    arrived(sv_r, str_.at[6])
    for k in range(7):
        t_two = t_two + sv_r[k]
    mean_in = jnp.sum(t_two[0:1, :], axis=1, keepdims=True)
    mean_out = jnp.sum(t_two[1:2, :], axis=1, keepdims=True)
    nmi_out[...] = min_v[...] - scaled_in * (STEP * jnp.sqrt(mean_in))
    nmo_out[...] = mout_v[...] - scaled_out * (STEP * jnp.sqrt(mean_out))
    for ref in (stw.at[0], hy_r, sx_r, hx_r, sz_r):
        arrived(ref, sts)
    arrived(sy_r, sts)
    arrived(sv_r, sts)


def put_out(ig, nmi, nmo, ig_out, nmi_out, nmo_out, sem):
    copies = [
        pltpu.make_async_copy(s, d, sem.at[i]) for i, (s, d) in enumerate(((nmi, nmi_out), (nmo, nmo_out), (ig, ig_out)))
    ]
    for cp in copies:
        cp.start()
    for cp in copies:
        cp.wait()


def body(
    inputs, pre_act, out_grad, w_in, w_out, master_in, master_out, row_in, col_in, row_out, col_out
):
    dma = pltpu.SemaphoreType.DMA
    vm = pltpu.VMEM
    shapes = (
        jax.ShapeDtypeStruct((OUTC, TOK), BF),
        jax.ShapeDtypeStruct((HID, COLS), F32),
        jax.ShapeDtypeStruct((HID, COLS), F32),
    )
    made = pl.pallas_call(
        kernel,
        name="backward_step",
        out_shape=shapes,
        in_specs=[pl.BlockSpec(memory_space=pl.ANY)] * 11,
        out_specs=[pl.BlockSpec(memory_space=pltpu.VMEM)] * 3,
        scratch_shapes=[
            vm((HID, TOK), BF), vm((TOK, D), BF), vm((HID, D), BF), vm((HID, D), BF),
            vm((HID, COLS), F32), vm((HID, COLS), F32),
            vm((COLS,), F32), vm((1, HID), F32), vm((1, HID), F32), vm((COLS,), F32),
            vm((2, 4, 4, 8, RT, COLS), BF), vm((2, HID, 2048), BF), vm((TOK, HID), BF),
            vm((TOK, 768), F32), vm((4, TOK, 768), BF), vm((4, TOK, 768), BF),
            vm((3, TOK, 768), BF), vm((3, TOK, 768), BF), vm((4, 2 * OUTC, TOK), BF), vm((8, 2 * OUTC, TOK), BF),
            vm((OUTC, TOK), BF), vm((RT, D), BF),
            vm((2, 256, 128), F32), vm((4, 8, 128), F32), vm((2, 8, 128), F32),
            vm((8, 128), F32), vm((7, 8, 128), F32), vm((7, 8, 128), F32), vm((7, 2, 128), F32),
            vm((8, 2, 128), F32), vm((7, 2, 128), F32), vm((7, 8, 128), F32), vm((8, 128), F32),
            dma((8,)), dma((PARTS,)), dma, dma((2,)), dma, dma((2,)),
            dma, dma((2, 14)), dma, dma((2, 14)), dma, dma((4,)), dma, dma((2,)),
            dma, dma((4,)), dma, dma, dma, dma, dma, dma, dma, dma((7,)), dma,
        ],
        compiler_params=pltpu.CompilerParams(
            collective_id=0, has_side_effects=True, vmem_limit_bytes=48 * 2**20
        ),
    )(
        *(
            pltpu.with_memory_space_constraint(v, pltpu.HBM)
            for v in (
                inputs, pre_act.T, out_grad, w_in.T, w_out, master_in.T, master_out,
                row_in, col_in.reshape(1, HID), row_out.reshape(1, HID), col_out,
            )
        )
    )
    out = pl.pallas_call(
        put_out,
        name="put_out",
        out_shape=shapes,
        in_specs=[pl.BlockSpec(memory_space=pl.ANY)] * 3,
        out_specs=[pl.BlockSpec(memory_space=pl.ANY)] * 3,
        scratch_shapes=[dma((3,))],
        compiler_params=pltpu.CompilerParams(vmem_limit_bytes=2**20),
    )(*made)
    return out[0].T, out[1].T, out[2]


def solution(mesh):
    return jax.shard_map(
        body,
        mesh=mesh,
        in_specs=(
            P("dp", None),
            P("dp", "mp"),
            P("dp", None),
            P(None, "mp"),
            P("mp", None),
            P("dp", "mp"),
            P("mp", "dp"),
            P("dp"),
            P("mp"),
            P("mp"),
            P("dp"),
        ),
        out_specs=(P("dp", "mp"), P("dp", "mp"), P("mp", "dp")),
        check_vma=False,
    )
```
